32 devices in a mesh: cells: 8 (over z, y), members: 4 (over x, core).
Axes of the slice: x: 2, y: 2, z: 4, core: 2. Of those that a mesh axis runs over, the one named last changes fastest.
Arguments:
- tmax: float32 [16, 97, 32768], P('members', None, 'cells'), may hold values from -24 to 24
- threshold: int32 [32768], P('cells'), may hold values from 0 to 79
- land_mask: int32 [32768], P('cells'), may hold values from 0 to 1, as said below
- region_id: int32 [32768], P('cells'), may hold values from 0 to 45, as said below
- block_fill: int32 [256], P('cells'), may hold values from 64 to 128
- cell_area: float32 [32768], P('cells'), may hold values from 0.1 to 1
Outputs:
- region_index: float32 [16, 92, 46], P('members')
- cell_mean: float32 [92, 32768], P('members', 'cells')
- land_count: int32 [46], replicated
The draws below stay inside these ranges and needn't reach their ends.
Inputs may be any that keep to these rules, and one draw needn't show every extreme that they name: `land_mask`: in every block of 128 slots the first 46 slots are land. `region_id`: in every block of 128 slots the first 46 slots name every region once.
All inputs are finite; a program needn't handle non-finite values.
Results may differ from the reference program's by a relative error of at most 0.0003.
Values sent between devices are 32-bit elements; how exact they have to be, the bound alone decides.
A program may use at most 64 MiB of HBM per device.

```python
import math
import jax
import jax.numpy as jnp
from jax import lax

MEMBERS = 16
DAYS = 92
WINDOW = 6
INPUT_DAYS = 97
REGIONS = 46
BLOCK = 128
BLOCKS = 256
CELLS = 32768


def draw_land_mask(key, part):
    index = jnp.arange(CELLS, dtype=jnp.int32)
    chance = 300 + 650 * index // CELLS
    rolls = jax.random.randint(jax.random.fold_in(key, 11), (CELLS,), 0, 1000)
    land = (rolls < chance).astype(jnp.int32)
    forced = (index % BLOCK < REGIONS).astype(jnp.int32)
    return jnp.maximum(land, forced)


def draw_region_id(key, part):
    index = jnp.arange(CELLS, dtype=jnp.int32)
    position = index % BLOCK
    shifts = jax.random.randint(jax.random.fold_in(key, 21), (BLOCKS,), 0, REGIONS)
    shift = jnp.repeat(shifts, BLOCK)
    covered = (position + shift) % REGIONS
    loose = jax.random.randint(jax.random.fold_in(key, 22), (CELLS,), 0, REGIONS)
    return jnp.where(position < REGIONS, covered, loose).astype(jnp.int32)


def place_ends(values, stream_key, smallest, top_value):
    extent = values.shape
    spot = [jax.random.randint(jax.random.fold_in(stream_key, axis), (), 0, extent[axis]) for axis in range(len(extent))]
    values = values.at[tuple(spot)].set(smallest)
    longest = extent.index(max(extent))
    spot[longest] = (spot[longest] + 1) % extent[longest]
    return values.at[tuple(spot)].set(top_value)


def block_levels(stream_key, dims, split, least, largest):
    def one(dim, shards_of):
        steps = jax.random.uniform(jax.random.fold_in(jax.random.fold_in(stream_key, 6), dim), (shards_of,), jnp.float32, least / len(split), largest / len(split))
        return jnp.repeat(jnp.exp(steps), dims[dim] // shards_of).reshape((-1,) + (1,) * (len(dims) - dim - 1))

    factor_of = one(*split[0])
    for cut in split[1:]:
        factor_of = factor_of * one(*cut)
    return factor_of


def noise(own_key, extent, spread, bound, split=(), held_as=jnp.bfloat16):
    values = spread * jax.random.normal(own_key, extent, jnp.float32)
    if split:
        values = values * block_levels(own_key, extent, split, -0.22, 0.18)
    return jnp.clip(values, -bound, bound).astype(held_as)


def setup_inputs(seed: int = 0) -> dict:
    seeds = jax.random.split(jax.random.key(seed), 7)
    tmax = noise(seeds[0], (MEMBERS, INPUT_DAYS, CELLS), 4.0, 24.0, ((0, 4), (2, 8)), jnp.float32)
    threshold = place_ends(jax.random.randint(seeds[1], (CELLS,), 0, 80), jax.random.fold_in(seeds[1], 1), 0, 79).astype(jnp.int32)
    land_mask = draw_land_mask(jax.random.fold_in(seeds[6], 71), 0)
    region_id = draw_region_id(jax.random.fold_in(seeds[6], 71), 0)
    block_fill = place_ends(jax.random.randint(seeds[4], (BLOCKS,), BLOCK // 2, BLOCK + 1), jax.random.fold_in(seeds[4], 1), BLOCK // 2, BLOCK).astype(jnp.int32)
    cell_area = jnp.clip(jnp.exp(math.log(1.0) - 2.3025851 * jax.random.uniform(seeds[5], (CELLS,), jnp.float32) ** block_levels(seeds[5], (CELLS,), ((0, 8),), -0.2, 0.2)), 0.1, 1.0)
    return dict(tmax=tmax, threshold=threshold, land_mask=land_mask, region_id=region_id, block_fill=block_fill, cell_area=cell_area)


def reference(tmax, threshold, land_mask, region_id, block_fill, cell_area):
    position = jnp.arange(CELLS, dtype=jnp.int32) % BLOCK
    filled = jnp.repeat(block_fill, BLOCK)
    live = land_mask * (position < filled).astype(jnp.int32)
    weight = cell_area * live.astype(jnp.float32)
    matches = region_id[:, None] == jnp.arange(REGIONS, dtype=jnp.int32)[None, :]
    onehot = matches.astype(jnp.float32)
    area_sum = jnp.dot(weight, onehot, precision=lax.Precision.HIGHEST)
    land_count = jnp.sum(live[:, None] * matches.astype(jnp.int32), axis=0)
    limit = threshold.astype(jnp.float32) * 0.1

    def one_member(total, member):
        excess = jnp.maximum(member - limit[None, :], 0.0)
        rolled = excess[0:DAYS]
        for shift in range(1, WINDOW):
            rolled = rolled + excess[shift:shift + DAYS]
        rolled = rolled / WINDOW
        sums = jnp.dot(rolled * weight[None, :], onehot, precision=lax.Precision.HIGHEST)
        return total + rolled, sums / area_sum[None, :]

    start = jnp.zeros((DAYS, CELLS), jnp.float32)
    total, region_index = lax.scan(one_member, start, tmax)
    cell_mean = live.astype(jnp.float32)[None, :] * total / MEMBERS
    return region_index, cell_mean, land_count
```

```python
import functools

import jax
import jax.numpy as jnp
from jax import lax
from jax.experimental import pallas as pl
from jax.experimental.pallas import tpu as pltpu
from jax.sharding import PartitionSpec as P

WINDOW = 6
REGIONS = 46
LANES = 128
TILES = 4
LAG = 3
QUARTERS = 4
MESH = pl.DeviceIdType.MESH


def up(n, step):
    return -(-n // step) * step


def kernel(
    dims,
    tmax_ref, thr_ref, land_ref, rid_ref, fill_ref, area_ref,
    region_ref, mean_ref, count_ref,
    x_buf, lhs, lhs_w, onehot, acc, acc_w, live_buf, s_buf, parts, got1, send2, got2,
    ep, rs_src, rs_got, mid_src, mid_got, whole,
    hbm_sem, s1_send, s1_recv, s2_send, s2_recv,
    rs_send, rs_recv, mid_send, mid_recv, ag_send, ag_recv,
):
    (members_here, in_days, days, chunks, width, slots, slot_rows, rows_out,
     pairs, share_rows, shares, groups, ensemble) = dims
    me_c = lax.axis_index("cells")
    me_m = lax.axis_index("members")
    group, mine = lax.div(me_c, shares), lax.rem(me_c, shares)
    side, core = lax.div(me_m, 2), lax.rem(me_m, 2)
    partner = side * 2 + (1 - core)
    across = (1 - side) * 2 + core

    def share_peer(k):
        return group * shares + lax.rem(mine + k, shares)

    def group_peer(k):
        return lax.rem(group + k, groups) * shares + mine

    barrier = pltpu.get_barrier_semaphore()
    for m in (partner, across):
        pl.semaphore_signal(barrier, inc=1, device_id={"members": m}, device_id_type=MESH)
    for k in range(1, shares):
        pl.semaphore_signal(barrier, inc=1, device_id={"cells": share_peer(k)}, device_id_type=MESH)
    for k in range(1, groups):
        pl.semaphore_signal(barrier, inc=1, device_id={"cells": group_peer(k)}, device_id_type=MESH)

    def load(c):
        return pltpu.make_async_copy(
            tmax_ref.at[:, :, pl.ds(c * width, width)], x_buf.at[c], hbm_sem.at[c]
        )

    for c in range(chunks):
        load(c).start()

    def copy1(c):
        return pltpu.make_async_remote_copy(
            src_ref=parts.at[c, 1 - core], dst_ref=got1.at[c],
            send_sem=s1_send.at[c], recv_sem=s1_recv.at[c],
            device_id={"members": partner}, device_id_type=MESH,
        )

    def copy2(c):
        return pltpu.make_async_remote_copy(
            src_ref=send2.at[c], dst_ref=got2.at[c],
            send_sem=s2_send.at[c], recv_sem=s2_recv.at[c],
            device_id={"members": across}, device_id_type=MESH,
        )

    region_rows = up(REGIONS, 16)
    onehot[...] = jnp.zeros_like(onehot)
    lhs[...] = jnp.zeros_like(lhs)
    acc[...] = jnp.zeros_like(acc)
    acc_w[...] = jnp.zeros_like(acc_w)
    ep[...] = jnp.zeros_like(ep)

    contract = (((1,), (1,)), ((), ()))

    def compute(c):
        at = pl.ds(pl.multiple_of(c * width, width), width)
        lane = lax.broadcasted_iota(jnp.int32, (1, LANES), 1)
        inside = jnp.concatenate(
            [(lane < fill_ref[c * TILES + j]).astype(jnp.int32) for j in range(TILES)], axis=1
        )
        live = (land_ref[:, at] * inside).astype(jnp.float32)
        live_buf[c] = live
        weight = area_ref[:, at] * live
        limit = thr_ref[:, at].astype(jnp.float32) * 0.1
        names = lax.broadcasted_iota(jnp.int32, (region_rows, width), 0)
        hot = jnp.where(names == rid_ref[:, at], 1.0, 0.0)
        onehot[0:region_rows, :] = hot.astype(jnp.bfloat16)
        line = lax.broadcasted_iota(jnp.int32, (16, width), 0)
        w_high = weight.astype(jnp.bfloat16).astype(jnp.float32)
        lhs_w[...] = jnp.where(
            line == 0, w_high,
            jnp.where(line == 1, weight - w_high, jnp.where(line == 2, live, 0.0)),
        ).astype(jnp.bfloat16)
        load(c).wait()
        total = None
        for m in range(members_here):
            excess = jnp.maximum(x_buf[c, m] - limit, 0.0)
            total = excess if total is None else total + excess
            weighted = excess * weight
            high = weighted.astype(jnp.bfloat16)
            low = (weighted - high.astype(jnp.float32)).astype(jnp.bfloat16)
            lhs[m, 0:in_days, :] = high
            lhs[m, slot_rows : slot_rows + in_days, :] = low
            acc[m] += lax.dot_general(
                lhs[m], onehot[...], contract, preferred_element_type=jnp.float32
            )
        s_buf[...] = total
        for d in range(4):
            lo = d * rows_out
            two = s_buf[lo : lo + rows_out + 4] + s_buf[lo + 1 : lo + rows_out + 5]
            parts[c, d % 2, d // 2] = two[0:rows_out] + two[2 : rows_out + 2] + two[4 : rows_out + 4]
        acc_w[...] += lax.dot_general(
            lhs_w[...], onehot[...], contract, preferred_element_type=jnp.float32
        )

    def cross(c):
        copy1(c).wait_recv()
        send2[c] = parts[c, core, 1 - side] + got1[c, 1 - side]
        copy2(c).start()

    compute(0)
    pl.semaphore_wait(barrier, 2 + (shares - 1) + (groups - 1))
    copy1(0).start()

    def step(c, carry):
        compute(c)
        copy1(c).start()

        @pl.when(c >= LAG)
        def _():
            cross(c - LAG)

        return carry

    lax.fori_loop(1, chunks, step, 0)

    def of_member(m):
        return acc[m, 0:in_days] + acc[m, slot_rows : slot_rows + in_days]

    for p in range(pairs):
        ep[p, 0:in_days] = of_member(2 * p) + pltpu.roll(of_member(2 * p + 1), LANES // 2, 1)
    area_row = acc_w[0:1] + acc_w[1:2]
    count_row = acc_w[2:3]
    line = lax.broadcasted_iota(jnp.int32, (share_rows, LANES), 0)
    for p in range(pairs):
        for q in range(QUARTERS):
            lo = q * share_rows
            rolled = ep[p, lo : lo + share_rows]
            for k in range(1, WINDOW):
                rolled = rolled + ep[p, lo + k : lo + k + share_rows]
            rolled = rolled / WINDOW
            for row, value in ((days, area_row), (days + 1, count_row)):
                if lo <= row < lo + share_rows:
                    rolled = jnp.where(line == row - lo, value, rolled)
            rs_src[p * QUARTERS + q] = rolled

    def rs_copy(k):
        return pltpu.make_async_remote_copy(
            src_ref=rs_src.at[lax.rem(mine + k, shares)], dst_ref=rs_got.at[k - 1],
            send_sem=rs_send.at[k - 1], recv_sem=rs_recv.at[k - 1],
            device_id={"cells": share_peer(k)}, device_id_type=MESH,
        )

    def mid_copy(k):
        return pltpu.make_async_remote_copy(
            src_ref=mid_src, dst_ref=mid_got.at[k - 1],
            send_sem=mid_send.at[k - 1], recv_sem=mid_recv.at[k - 1],
            device_id={"cells": group_peer(k)}, device_id_type=MESH,
        )

    def ag_copy(k):
        return pltpu.make_async_remote_copy(
            src_ref=whole.at[mine], dst_ref=whole.at[mine],
            send_sem=ag_send.at[k - 1], recv_sem=ag_recv.at[k - 1],
            device_id={"cells": share_peer(k)}, device_id_type=MESH,
        )

    for k in range(1, shares):
        rs_copy(k).start()
    for c in range(max(chunks - LAG, 0), chunks):
        cross(c)
    own = rs_src[mine]
    for k in range(1, shares):
        rs_copy(k).wait_recv()
        own = own + rs_got[k - 1]
    if groups > 1:
        mid_src[...] = own
        for k in range(1, groups):
            mid_copy(k).start()
        for k in range(1, groups):
            mid_copy(k).wait_recv()
            own = own + mid_got[k - 1]
    whole[mine] = own
    for k in range(1, shares):
        ag_copy(k).start()

    def finish(c):
        copy2(c).wait_recv()
        at = slice(c * width, (c + 1) * width)
        total = parts[c, core, side] + got1[c, side] + got2[c]
        mean_ref[:, at] = total * live_buf[c] / (WINDOW * ensemble)

    late = chunks - 2
    for c in range(late):
        finish(c)
    for k in range(1, shares):
        ag_copy(k).wait_recv()
    all_shares = whole[...]
    spot = lambda row: all_shares[row // share_rows, row % share_rows : row % share_rows + 1]
    area = spot(days)
    count_ref[...] = spot(days + 1)[:, 0:REGIONS].astype(jnp.int32)
    for p in range(pairs):
        sums = all_shares[p * QUARTERS : (p + 1) * QUARTERS].reshape(QUARTERS * share_rows, LANES)
        region_ref[2 * p] = sums[0:days, 0:REGIONS] / area[:, 0:REGIONS]
        sums = pltpu.roll(sums, LANES // 2, 1)
        region_ref[2 * p + 1] = sums[0:days, 0:REGIONS] / area[:, 0:REGIONS]
    for c in range(late, chunks):
        finish(c)
    for c in range(chunks):
        copy1(c).wait_send()
        copy2(c).wait_send()
    for k in range(1, shares):
        rs_copy(k).wait_send()
        ag_copy(k).wait_send()
    for k in range(1, groups):
        mid_copy(k).wait_send()


def shards(n_cells, n_members, tmax, threshold, land_mask, region_id, block_fill, cell_area):
    members_here, in_days, cell_dev = tmax.shape
    days = in_days - WINDOW + 1
    slots = cell_dev // block_fill.shape[0]
    assert slots == LANES and n_members == 4 and members_here % 2 == 0
    width = TILES * slots
    chunks = cell_dev // width
    slot_rows = up(in_days, 16)
    rows_out = days // n_members
    pairs = members_here // 2
    share_rows = up(-(-(days + 2) // QUARTERS), 8)
    shares = pairs * QUARTERS
    groups = n_cells // shares
    ensemble = n_members * members_here
    dims = (members_here, in_days, days, chunks, width, slots, slot_rows, rows_out,
            pairs, share_rows, shares, groups, ensemble)
    f32, bf16 = jnp.float32, jnp.bfloat16
    dma = pltpu.SemaphoreType.DMA
    vmem = pl.BlockSpec(memory_space=pltpu.VMEM)
    others = max(groups - 1, 1)
    ep_rows = up(QUARTERS * share_rows + WINDOW - 1, 8)
    row = lambda v: v.reshape(1, cell_dev)
    region, mean, count = pl.pallas_call(
        functools.partial(kernel, dims),
        name="warm_spell",
        out_shape=(
            jax.ShapeDtypeStruct((members_here, days, REGIONS), f32),
            jax.ShapeDtypeStruct((rows_out, cell_dev), f32),
            jax.ShapeDtypeStruct((1, REGIONS), jnp.int32),
        ),
        in_specs=[
            pl.BlockSpec(memory_space=pl.ANY), vmem, vmem, vmem,
            pl.BlockSpec(memory_space=pltpu.SMEM), vmem,
        ],
        out_specs=(vmem, vmem, vmem),
        scratch_shapes=[
            pltpu.VMEM((chunks, members_here, in_days, width), f32),
            pltpu.VMEM((members_here, 2 * slot_rows, width), bf16),
            pltpu.VMEM((16, width), bf16),
            pltpu.VMEM((LANES, width), bf16),
            pltpu.VMEM((members_here, 2 * slot_rows, LANES), f32),
            pltpu.VMEM((16, LANES), f32),
            pltpu.VMEM((chunks, 1, width), f32),
            pltpu.VMEM((in_days, width), f32),
            pltpu.VMEM((chunks, 2, 2, rows_out, width), f32),
            pltpu.VMEM((chunks, 2, rows_out, width), f32),
            pltpu.VMEM((chunks, rows_out, width), f32),
            pltpu.VMEM((chunks, rows_out, width), f32),
            pltpu.VMEM((pairs, ep_rows, LANES), f32),
            pltpu.VMEM((shares, share_rows, LANES), f32),
            pltpu.VMEM((shares - 1, share_rows, LANES), f32),
            pltpu.VMEM((share_rows, LANES), f32),
            pltpu.VMEM((others, share_rows, LANES), f32),
            pltpu.VMEM((shares, share_rows, LANES), f32),
            dma((chunks,)), dma((chunks,)), dma((chunks,)), dma((chunks,)), dma((chunks,)),
            dma((shares - 1,)), dma((shares - 1,)), dma((others,)), dma((others,)),
            dma((shares - 1,)), dma((shares - 1,)),
        ],
        compiler_params=pltpu.CompilerParams(
            collective_id=0, has_side_effects=True, vmem_limit_bytes=48 * 1024 * 1024
        ),
    )(tmax, row(threshold), row(land_mask), row(region_id), block_fill, row(cell_area))
    return region, mean, count.reshape(REGIONS)


def solution(mesh):
    body = functools.partial(shards, mesh.shape["cells"], mesh.shape["members"])
    return jax.shard_map(
        body,
        mesh=mesh,
        in_specs=(
            P("members", None, "cells"),
            P("cells"),
            P("cells"),
            P("cells"),
            P("cells"),
            P("cells"),
        ),
        out_specs=(P("members", None, None), P("members", "cells"), P()),
        check_vma=False,
    )
```

```python
import functools

import jax
import jax.numpy as jnp
from jax import lax
from jax.experimental import pallas as pl
from jax.experimental.pallas import tpu as pltpu
from jax.sharding import PartitionSpec as P

WINDOW = 6
REGIONS = 46
LANES = 128
TILES = 4
LAG = 3
QUARTERS = 4
MESH = pl.DeviceIdType.MESH


def up(n, step):
    return -(-n // step) * step


def kernel(
    dims,
    tmax_ref, thr_ref, land_ref, rid_ref, fill_ref, area_ref,
    region_ref, mean_ref, count_ref,
    x_buf, lhs, lhs_w, onehot, acc, acc_w, live_buf, s_buf, parts, got1, send2, got2,
    ep, rs_src, rs_got, mid_src, mid_got, whole,
    hbm_sem, s1_send, s1_recv, s2_send, s2_recv,
    rs_send, rs_recv, mid_send, mid_recv, ag_send, ag_recv,
):
    (members_here, in_days, days, chunks, width, slots, slot_rows, rows_out,
     pairs, share_rows, shares, groups, ensemble) = dims
    me_c = lax.axis_index("cells")
    me_m = lax.axis_index("members")
    group, mine = lax.div(me_c, shares), lax.rem(me_c, shares)
    side, core = lax.div(me_m, 2), lax.rem(me_m, 2)
    partner = side * 2 + (1 - core)
    across = (1 - side) * 2 + core

    def share_peer(k):
        return group * shares + lax.rem(mine + k, shares)

    def group_peer(k):
        return lax.rem(group + k, groups) * shares + mine

    barrier = pltpu.get_barrier_semaphore()
    for m in (partner, across):
        pl.semaphore_signal(barrier, inc=1, device_id={"members": m}, device_id_type=MESH)
    for k in range(1, shares):
        pl.semaphore_signal(barrier, inc=1, device_id={"cells": share_peer(k)}, device_id_type=MESH)
    for k in range(1, groups):
        pl.semaphore_signal(barrier, inc=1, device_id={"cells": group_peer(k)}, device_id_type=MESH)

    rows = TILES * members_here
    in_rows = x_buf.shape[1]
    x_flat = x_buf.reshape(chunks * in_rows * rows, LANES)

    def days_of(c, m):
        return jnp.concatenate(
            [
                x_flat[pl.ds(c * (in_rows * rows) + j * members_here + m, in_rows, stride=rows), :]
                for j in range(TILES)
            ],
            axis=1,
        )

    def load(c):
        return pltpu.make_async_copy(
            tmax_ref.at[:, pl.ds(c * rows, rows), :], x_buf.at[c, pl.ds(0, in_days)], hbm_sem.at[c]
        )

    for c in range(chunks):
        load(c).start()

    def copy1(c):
        return pltpu.make_async_remote_copy(
            src_ref=parts.at[c, 1 - core], dst_ref=got1.at[c],
            send_sem=s1_send.at[c], recv_sem=s1_recv.at[c],
            device_id={"members": partner}, device_id_type=MESH,
        )

    def copy2(c):
        return pltpu.make_async_remote_copy(
            src_ref=send2.at[c], dst_ref=got2.at[c],
            send_sem=s2_send.at[c], recv_sem=s2_recv.at[c],
            device_id={"members": across}, device_id_type=MESH,
        )

    region_rows = up(REGIONS, 16)
    onehot[...] = jnp.zeros_like(onehot)
    lhs[...] = jnp.zeros_like(lhs)
    acc[...] = jnp.zeros_like(acc)
    acc_w[...] = jnp.zeros_like(acc_w)
    ep[...] = jnp.zeros_like(ep)

    contract = (((1,), (1,)), ((), ()))

    def compute(c):
        at = pl.ds(pl.multiple_of(c * width, width), width)
        lane = lax.broadcasted_iota(jnp.int32, (1, LANES), 1)
        inside = jnp.concatenate(
            [(lane < fill_ref[c * TILES + j]).astype(jnp.int32) for j in range(TILES)], axis=1
        )
        live = (land_ref[:, at] * inside).astype(jnp.float32)
        live_buf[c] = live
        weight = area_ref[:, at] * live
        limit = thr_ref[:, at].astype(jnp.float32) * 0.1
        names = lax.broadcasted_iota(jnp.int32, (region_rows, width), 0)
        hot = jnp.where(names == rid_ref[:, at], 1.0, 0.0)
        onehot[0:region_rows, :] = hot.astype(jnp.bfloat16)
        line = lax.broadcasted_iota(jnp.int32, (16, width), 0)
        w_high = weight.astype(jnp.bfloat16).astype(jnp.float32)
        lhs_w[...] = jnp.where(
            line == 0, w_high,
            jnp.where(line == 1, weight - w_high, jnp.where(line == 2, live, 0.0)),
        ).astype(jnp.bfloat16)
        load(c).wait()
        total = None
        for m in range(members_here):
            excess = jnp.maximum(days_of(c, m) - limit, 0.0)
            total = excess if total is None else total + excess
            weighted = excess * weight
            high = weighted.astype(jnp.bfloat16)
            low = (weighted - high.astype(jnp.float32)).astype(jnp.bfloat16)
            lhs[m, 0:in_rows, :] = high
            lhs[m, slot_rows : slot_rows + in_rows, :] = low
            acc[m] += lax.dot_general(
                lhs[m], onehot[...], contract, preferred_element_type=jnp.float32
            )
        s_buf[...] = total
        for d in range(4):
            lo = d * rows_out
            two = s_buf[lo : lo + rows_out + 4] + s_buf[lo + 1 : lo + rows_out + 5]
            parts[c, d % 2, d // 2] = two[0:rows_out] + two[2 : rows_out + 2] + two[4 : rows_out + 4]
        acc_w[...] += lax.dot_general(
            lhs_w[...], onehot[...], contract, preferred_element_type=jnp.float32
        )

    def cross(c):
        copy1(c).wait_recv()
        send2[c] = parts[c, core, 1 - side] + got1[c, 1 - side]
        copy2(c).start()

    compute(0)
    pl.semaphore_wait(barrier, 2 + (shares - 1) + (groups - 1))
    copy1(0).start()

    def step(c, carry):
        compute(c)
        copy1(c).start()

        @pl.when(c >= LAG)
        def _():
            cross(c - LAG)

        return carry

    lax.fori_loop(1, chunks, step, 0)

    def of_member(m):
        return acc[m, 0:in_days] + acc[m, slot_rows : slot_rows + in_days]

    for p in range(pairs):
        ep[p, 0:in_days] = of_member(2 * p) + pltpu.roll(of_member(2 * p + 1), LANES // 2, 1)
    area_row = acc_w[0:1] + acc_w[1:2]
    count_row = acc_w[2:3]
    line = lax.broadcasted_iota(jnp.int32, (share_rows, LANES), 0)
    for p in range(pairs):
        for q in range(QUARTERS):
            lo = q * share_rows
            rolled = ep[p, lo : lo + share_rows]
            for k in range(1, WINDOW):
                rolled = rolled + ep[p, lo + k : lo + k + share_rows]
            rolled = rolled / WINDOW
            for row, value in ((days, area_row), (days + 1, count_row)):
                if lo <= row < lo + share_rows:
                    rolled = jnp.where(line == row - lo, value, rolled)
            rs_src[p * QUARTERS + q] = rolled

    def rs_copy(k):
        return pltpu.make_async_remote_copy(
            src_ref=rs_src.at[lax.rem(mine + k, shares)], dst_ref=rs_got.at[k - 1],
            send_sem=rs_send.at[k - 1], recv_sem=rs_recv.at[k - 1],
            device_id={"cells": share_peer(k)}, device_id_type=MESH,
        )

    def mid_copy(k):
        return pltpu.make_async_remote_copy(
            src_ref=mid_src, dst_ref=mid_got.at[k - 1],
            send_sem=mid_send.at[k - 1], recv_sem=mid_recv.at[k - 1],
            device_id={"cells": group_peer(k)}, device_id_type=MESH,
        )

    def ag_copy(k):
        return pltpu.make_async_remote_copy(
            src_ref=whole.at[mine], dst_ref=whole.at[mine],
            send_sem=ag_send.at[k - 1], recv_sem=ag_recv.at[k - 1],
            device_id={"cells": share_peer(k)}, device_id_type=MESH,
        )

    for k in range(1, shares):
        rs_copy(k).start()
    for c in range(max(chunks - LAG, 0), chunks):
        cross(c)
    own = rs_src[mine]
    for k in range(1, shares):
        rs_copy(k).wait_recv()
        own = own + rs_got[k - 1]
    if groups > 1:
        mid_src[...] = own
        for k in range(1, groups):
            mid_copy(k).start()
        for k in range(1, groups):
            mid_copy(k).wait_recv()
            own = own + mid_got[k - 1]
    whole[mine] = own
    for k in range(1, shares):
        ag_copy(k).start()

    def finish(c):
        copy2(c).wait_recv()
        at = slice(c * width, (c + 1) * width)
        total = parts[c, core, side] + got1[c, side] + got2[c]
        mean_ref[:, at] = total * live_buf[c] / (WINDOW * ensemble)

    late = chunks - 2
    for c in range(late):
        finish(c)
    for k in range(1, shares):
        ag_copy(k).wait_recv()
    all_shares = whole[...]
    spot = lambda row: all_shares[row // share_rows, row % share_rows : row % share_rows + 1]
    area = spot(days)
    count_ref[...] = spot(days + 1)[:, 0:REGIONS].astype(jnp.int32)
    for p in range(pairs):
        sums = all_shares[p * QUARTERS : (p + 1) * QUARTERS].reshape(QUARTERS * share_rows, LANES)
        region_ref[2 * p] = sums[0:days, 0:REGIONS] / area[:, 0:REGIONS]
        sums = pltpu.roll(sums, LANES // 2, 1)
        region_ref[2 * p + 1] = sums[0:days, 0:REGIONS] / area[:, 0:REGIONS]
    for c in range(late, chunks):
        finish(c)
    for c in range(chunks):
        copy1(c).wait_send()
        copy2(c).wait_send()
    for k in range(1, shares):
        rs_copy(k).wait_send()
        ag_copy(k).wait_send()
    for k in range(1, groups):
        mid_copy(k).wait_send()


def shards(n_cells, n_members, tmax, threshold, land_mask, region_id, block_fill, cell_area):
    members_here, in_days, cell_dev = tmax.shape
    days = in_days - WINDOW + 1
    slots = cell_dev // block_fill.shape[0]
    assert slots == LANES and n_members == 4 and members_here % 2 == 0
    width = TILES * slots
    chunks = cell_dev // width
    slot_rows, in_rows = up(in_days, 16), up(in_days, 8)
    rows_out = days // n_members
    pairs = members_here // 2
    share_rows = up(-(-(days + 2) // QUARTERS), 8)
    shares = pairs * QUARTERS
    groups = n_cells // shares
    ensemble = n_members * members_here
    dims = (members_here, in_days, days, chunks, width, slots, slot_rows, rows_out,
            pairs, share_rows, shares, groups, ensemble)
    f32, bf16 = jnp.float32, jnp.bfloat16
    dma = pltpu.SemaphoreType.DMA
    vmem = pl.BlockSpec(memory_space=pltpu.VMEM)
    others = max(groups - 1, 1)
    ep_rows = up(QUARTERS * share_rows + WINDOW - 1, 8)
    tiles = cell_dev // LANES
    view = tmax.transpose(1, 0, 2).reshape(in_days, members_here, tiles, LANES)
    view = view.transpose(0, 2, 1, 3).reshape(in_days, tiles * members_here, LANES)
    row = lambda v: v.reshape(1, cell_dev)
    region, mean, count = pl.pallas_call(
        functools.partial(kernel, dims),
        name="warm_spell",
        out_shape=(
            jax.ShapeDtypeStruct((members_here, days, REGIONS), f32),
            jax.ShapeDtypeStruct((rows_out, cell_dev), f32),
            jax.ShapeDtypeStruct((1, REGIONS), jnp.int32),
        ),
        in_specs=[
            pl.BlockSpec(memory_space=pl.ANY), vmem, vmem, vmem,
            pl.BlockSpec(memory_space=pltpu.SMEM), vmem,
        ],
        out_specs=(vmem, vmem, vmem),
        scratch_shapes=[
            pltpu.VMEM((chunks, in_rows, TILES * members_here, LANES), f32),
            pltpu.VMEM((members_here, 2 * slot_rows, width), bf16),
            pltpu.VMEM((16, width), bf16),
            pltpu.VMEM((LANES, width), bf16),
            pltpu.VMEM((members_here, 2 * slot_rows, LANES), f32),
            pltpu.VMEM((16, LANES), f32),
            pltpu.VMEM((chunks, 1, width), f32),
            pltpu.VMEM((in_rows, width), f32),
            pltpu.VMEM((chunks, 2, 2, rows_out, width), f32),
            pltpu.VMEM((chunks, 2, rows_out, width), f32),
            pltpu.VMEM((chunks, rows_out, width), f32),
            pltpu.VMEM((chunks, rows_out, width), f32),
            pltpu.VMEM((pairs, ep_rows, LANES), f32),
            pltpu.VMEM((shares, share_rows, LANES), f32),
            pltpu.VMEM((shares - 1, share_rows, LANES), f32),
            pltpu.VMEM((share_rows, LANES), f32),
            pltpu.VMEM((others, share_rows, LANES), f32),
            pltpu.VMEM((shares, share_rows, LANES), f32),
            dma((chunks,)), dma((chunks,)), dma((chunks,)), dma((chunks,)), dma((chunks,)),
            dma((shares - 1,)), dma((shares - 1,)), dma((others,)), dma((others,)),
            dma((shares - 1,)), dma((shares - 1,)),
        ],
        compiler_params=pltpu.CompilerParams(
            collective_id=0, has_side_effects=True, vmem_limit_bytes=48 * 1024 * 1024
        ),
    )(view, row(threshold), row(land_mask), row(region_id), block_fill, row(cell_area))
    return region, mean, count.reshape(REGIONS)


def solution(mesh):
    body = functools.partial(shards, mesh.shape["cells"], mesh.shape["members"])
    return jax.shard_map(
        body,
        mesh=mesh,
        in_specs=(
            P("members", None, "cells"),
            P("cells"),
            P("cells"),
            P("cells"),
            P("cells"),
            P("cells"),
        ),
        out_specs=(P("members", None, None), P("members", "cells"), P()),
        check_vma=False,
    )
```

```python
import functools

import jax
import jax.numpy as jnp
from jax import lax
from jax.experimental import pallas as pl
from jax.experimental.pallas import tpu as pltpu
from jax.sharding import PartitionSpec as P

WINDOW = 6
REGIONS = 46
LANES = 128
TILES = 4
LAG = 3
QUARTERS = 4
MESH = pl.DeviceIdType.MESH


def up(n, step):
    return -(-n // step) * step


def kernel(
    dims,
    tmax_ref, thr_hbm, land_hbm, rid_hbm, fill_hbm, area_hbm,
    region_ref, mean_ref, count_ref,
    thr_ref, land_ref, rid_ref, fill_ref, area_ref, x_buf, lhs, lhs_w, onehot, acc, acc_w, live_buf, s_buf, parts, got1, send2, got2,
    ep, rs_src, rs_got, mid_src, mid_got, whole,
    small_sem, hbm_sem, s1_send, s1_recv, s2_send, s2_recv,
    rs_send, rs_recv, mid_send, mid_recv, ag_send, ag_recv,
):
    (members_here, in_days, days, chunks, width, slots, slot_rows, rows_out,
     pairs, share_rows, shares, groups, ensemble) = dims
    me_c = lax.axis_index("cells")
    me_m = lax.axis_index("members")
    group, mine = lax.div(me_c, shares), lax.rem(me_c, shares)
    side, core = lax.div(me_m, 2), lax.rem(me_m, 2)
    partner = side * 2 + (1 - core)
    across = (1 - side) * 2 + core

    def share_peer(k):
        return group * shares + lax.rem(mine + k, shares)

    def group_peer(k):
        return lax.rem(group + k, groups) * shares + mine

    small = [
        pltpu.make_async_copy(src, dst, small_sem.at[n])
        for n, (src, dst) in enumerate((
            (rid_hbm, rid_ref), (fill_hbm, fill_ref), (land_hbm, land_ref),
            (area_hbm, area_ref), (thr_hbm, thr_ref),
        ))
    ]
    for copy in small:
        copy.start()
    barrier = pltpu.get_barrier_semaphore()
    for m in (partner, across):
        pl.semaphore_signal(barrier, inc=1, device_id={"members": m}, device_id_type=MESH)
    for k in range(1, shares):
        pl.semaphore_signal(barrier, inc=1, device_id={"cells": share_peer(k)}, device_id_type=MESH)
    for k in range(1, groups):
        pl.semaphore_signal(barrier, inc=1, device_id={"cells": group_peer(k)}, device_id_type=MESH)

    rows = TILES * members_here
    in_rows = x_buf.shape[1]
    x_flat = x_buf.reshape(chunks * in_rows * rows, LANES)

    def days_of(c, m):
        return jnp.concatenate(
            [
                x_flat[pl.ds(c * (in_rows * rows) + j * members_here + m, in_rows, stride=rows), :]
                for j in range(TILES)
            ],
            axis=1,
        )

    def load(c):
        return pltpu.make_async_copy(
            tmax_ref.at[:, pl.ds(c * rows, rows), :], x_buf.at[c, pl.ds(0, in_days)], hbm_sem.at[c]
        )

    load(0).start()
    load(1).start()

    def copy1(c):
        return pltpu.make_async_remote_copy(
            src_ref=parts.at[c, 1 - core], dst_ref=got1.at[c],
            send_sem=s1_send.at[c], recv_sem=s1_recv.at[c],
            device_id={"members": partner}, device_id_type=MESH,
        )

    def copy2(c):
        return pltpu.make_async_remote_copy(
            src_ref=send2.at[c], dst_ref=got2.at[c],
            send_sem=s2_send.at[c], recv_sem=s2_recv.at[c],
            device_id={"members": across}, device_id_type=MESH,
        )

    region_rows = up(REGIONS, 16)
    onehot[...] = jnp.zeros_like(onehot)
    lhs[...] = jnp.zeros_like(lhs)
    acc[...] = jnp.zeros_like(acc)
    acc_w[...] = jnp.zeros_like(acc_w)
    ep[...] = jnp.zeros_like(ep)

    contract = (((1,), (1,)), ((), ()))

    def compute(c):
        at = pl.ds(pl.multiple_of(c * width, width), width)
        lane = lax.broadcasted_iota(jnp.int32, (1, LANES), 1)
        inside = jnp.concatenate(
            [(lane < fill_ref[c * TILES + j]).astype(jnp.int32) for j in range(TILES)], axis=1
        )
        live = (land_ref[:, at] * inside).astype(jnp.float32)
        live_buf[c] = live
        weight = area_ref[:, at] * live
        limit = thr_ref[:, at].astype(jnp.float32) * 0.1
        names = lax.broadcasted_iota(jnp.int32, (region_rows, width), 0)
        hot = jnp.where(names == rid_ref[:, at], 1.0, 0.0)
        onehot[0:region_rows, :] = hot.astype(jnp.bfloat16)
        line = lax.broadcasted_iota(jnp.int32, (16, width), 0)
        w_high = weight.astype(jnp.bfloat16).astype(jnp.float32)
        lhs_w[...] = jnp.where(
            line == 0, w_high,
            jnp.where(line == 1, weight - w_high, jnp.where(line == 2, live, 0.0)),
        ).astype(jnp.bfloat16)
        load(c).wait()
        total = None
        for m in range(members_here):
            excess = jnp.maximum(days_of(c, m) - limit, 0.0)
            total = excess if total is None else total + excess
            weighted = excess * weight
            high = weighted.astype(jnp.bfloat16)
            low = (weighted - high.astype(jnp.float32)).astype(jnp.bfloat16)
            lhs[m, 0:in_rows, :] = high
            lhs[m, slot_rows : slot_rows + in_rows, :] = low
            acc[m] += lax.dot_general(
                lhs[m], onehot[...], contract, preferred_element_type=jnp.float32
            )
        s_buf[...] = total
        for d in range(4):
            lo = d * rows_out
            two = s_buf[lo : lo + rows_out + 4] + s_buf[lo + 1 : lo + rows_out + 5]
            parts[c, d % 2, d // 2] = two[0:rows_out] + two[2 : rows_out + 2] + two[4 : rows_out + 4]
        acc_w[...] += lax.dot_general(
            lhs_w[...], onehot[...], contract, preferred_element_type=jnp.float32
        )

    def cross(c):
        copy1(c).wait_recv()
        send2[c] = parts[c, core, 1 - side] + got1[c, 1 - side]
        copy2(c).start()

    for c in range(2, chunks):
        load(c).start()
    for copy in small:
        copy.wait()
    compute(0)
    pl.semaphore_wait(barrier, 2 + (shares - 1) + (groups - 1))
    copy1(0).start()

    def step(c, carry):
        compute(c)
        copy1(c).start()

        @pl.when(c >= LAG)
        def _():
            cross(c - LAG)

        return carry

    lax.fori_loop(1, chunks, step, 0)

    def of_member(m):
        return acc[m, 0:in_days] + acc[m, slot_rows : slot_rows + in_days]

    for p in range(pairs):
        ep[p, 0:in_days] = of_member(2 * p) + pltpu.roll(of_member(2 * p + 1), LANES // 2, 1)
    area_row = acc_w[0:1] + acc_w[1:2]
    count_row = acc_w[2:3]
    line = lax.broadcasted_iota(jnp.int32, (share_rows, LANES), 0)
    for p in range(pairs):
        for q in range(QUARTERS):
            lo = q * share_rows
            rolled = ep[p, lo : lo + share_rows]
            for k in range(1, WINDOW):
                rolled = rolled + ep[p, lo + k : lo + k + share_rows]
            rolled = rolled / WINDOW
            for row, value in ((days, area_row), (days + 1, count_row)):
                if lo <= row < lo + share_rows:
                    rolled = jnp.where(line == row - lo, value, rolled)
            rs_src[p * QUARTERS + q] = rolled

    def rs_copy(k):
        return pltpu.make_async_remote_copy(
            src_ref=rs_src.at[lax.rem(mine + k, shares)], dst_ref=rs_got.at[k - 1],
            send_sem=rs_send.at[k - 1], recv_sem=rs_recv.at[k - 1],
            device_id={"cells": share_peer(k)}, device_id_type=MESH,
        )

    def mid_copy(k):
        return pltpu.make_async_remote_copy(
            src_ref=mid_src, dst_ref=mid_got.at[k - 1],
            send_sem=mid_send.at[k - 1], recv_sem=mid_recv.at[k - 1],
            device_id={"cells": group_peer(k)}, device_id_type=MESH,
        )

    def ag_copy(k):
        return pltpu.make_async_remote_copy(
            src_ref=whole.at[mine], dst_ref=whole.at[mine],
            send_sem=ag_send.at[k - 1], recv_sem=ag_recv.at[k - 1],
            device_id={"cells": share_peer(k)}, device_id_type=MESH,
        )

    for k in range(1, shares):
        rs_copy(k).start()
    for c in range(max(chunks - LAG, 0), chunks):
        cross(c)
    own = rs_src[mine]
    for k in range(1, shares):
        rs_copy(k).wait_recv()
        own = own + rs_got[k - 1]
    if groups > 1:
        mid_src[...] = own
        for k in range(1, groups):
            mid_copy(k).start()
        for k in range(1, groups):
            mid_copy(k).wait_recv()
            own = own + mid_got[k - 1]
    whole[mine] = own
    for k in range(1, shares):
        ag_copy(k).start()

    def finish(c):
        copy2(c).wait_recv()
        at = slice(c * width, (c + 1) * width)
        total = parts[c, core, side] + got1[c, side] + got2[c]
        mean_ref[:, at] = total * live_buf[c] / (WINDOW * ensemble)

    late = chunks - 2
    for c in range(late):
        finish(c)
    for k in range(1, shares):
        ag_copy(k).wait_recv()
    all_shares = whole[...]
    spot = lambda row: all_shares[row // share_rows, row % share_rows : row % share_rows + 1]
    area = spot(days)
    count_ref[...] = spot(days + 1)[:, 0:REGIONS].astype(jnp.int32)
    for p in range(pairs):
        sums = all_shares[p * QUARTERS : (p + 1) * QUARTERS].reshape(QUARTERS * share_rows, LANES)
        region_ref[2 * p] = sums[0:days, 0:REGIONS] / area[:, 0:REGIONS]
        sums = pltpu.roll(sums, LANES // 2, 1)
        region_ref[2 * p + 1] = sums[0:days, 0:REGIONS] / area[:, 0:REGIONS]
    for c in range(late, chunks):
        finish(c)
    for c in range(chunks):
        copy1(c).wait_send()
        copy2(c).wait_send()
    for k in range(1, shares):
        rs_copy(k).wait_send()
        ag_copy(k).wait_send()
    for k in range(1, groups):
        mid_copy(k).wait_send()


def shards(n_cells, n_members, tmax, threshold, land_mask, region_id, block_fill, cell_area):
    members_here, in_days, cell_dev = tmax.shape
    days = in_days - WINDOW + 1
    slots = cell_dev // block_fill.shape[0]
    assert slots == LANES and n_members == 4 and members_here % 2 == 0
    width = TILES * slots
    chunks = cell_dev // width
    slot_rows, in_rows = up(in_days, 16), up(in_days, 8)
    rows_out = days // n_members
    pairs = members_here // 2
    share_rows = up(-(-(days + 2) // QUARTERS), 8)
    shares = pairs * QUARTERS
    groups = n_cells // shares
    ensemble = n_members * members_here
    dims = (members_here, in_days, days, chunks, width, slots, slot_rows, rows_out,
            pairs, share_rows, shares, groups, ensemble)
    f32, bf16 = jnp.float32, jnp.bfloat16
    dma = pltpu.SemaphoreType.DMA
    vmem = pl.BlockSpec(memory_space=pltpu.VMEM)
    others = max(groups - 1, 1)
    ep_rows = up(QUARTERS * share_rows + WINDOW - 1, 8)
    tiles = cell_dev // LANES
    view = tmax.transpose(1, 0, 2).reshape(in_days, members_here, tiles, LANES)
    view = view.transpose(0, 2, 1, 3).reshape(in_days, tiles * members_here, LANES)
    row = lambda v: v.reshape(1, cell_dev)
    region, mean, count = pl.pallas_call(
        functools.partial(kernel, dims),
        name="warm_spell",
        out_shape=(
            jax.ShapeDtypeStruct((members_here, days, REGIONS), f32),
            jax.ShapeDtypeStruct((rows_out, cell_dev), f32),
            jax.ShapeDtypeStruct((1, REGIONS), jnp.int32),
        ),
        in_specs=[
            pl.BlockSpec(memory_space=pltpu.HBM) for _ in range(6)
        ],
        out_specs=(vmem, vmem, vmem),
        scratch_shapes=[
            pltpu.VMEM((1, cell_dev), jnp.int32),
            pltpu.VMEM((1, cell_dev), jnp.int32),
            pltpu.VMEM((1, cell_dev), jnp.int32),
            pltpu.SMEM(block_fill.shape, jnp.int32),
            pltpu.VMEM((1, cell_dev), f32),
            pltpu.VMEM((chunks, in_rows, TILES * members_here, LANES), f32),
            pltpu.VMEM((members_here, 2 * slot_rows, width), bf16),
            pltpu.VMEM((16, width), bf16),
            pltpu.VMEM((LANES, width), bf16),
            pltpu.VMEM((members_here, 2 * slot_rows, LANES), f32),
            pltpu.VMEM((16, LANES), f32),
            pltpu.VMEM((chunks, 1, width), f32),
            pltpu.VMEM((in_rows, width), f32),
            pltpu.VMEM((chunks, 2, 2, rows_out, width), f32),
            pltpu.VMEM((chunks, 2, rows_out, width), f32),
            pltpu.VMEM((chunks, rows_out, width), f32),
            pltpu.VMEM((chunks, rows_out, width), f32),
            pltpu.VMEM((pairs, ep_rows, LANES), f32),
            pltpu.VMEM((shares, share_rows, LANES), f32),
            pltpu.VMEM((shares - 1, share_rows, LANES), f32),
            pltpu.VMEM((share_rows, LANES), f32),
            pltpu.VMEM((others, share_rows, LANES), f32),
            pltpu.VMEM((shares, share_rows, LANES), f32),
            dma((5,)), dma((chunks,)), dma((chunks,)), dma((chunks,)), dma((chunks,)), dma((chunks,)),
            dma((shares - 1,)), dma((shares - 1,)), dma((others,)), dma((others,)),
            dma((shares - 1,)), dma((shares - 1,)),
        ],
        compiler_params=pltpu.CompilerParams(
            collective_id=0, has_side_effects=True, vmem_limit_bytes=67043328
        ),
    )(view, row(threshold), row(land_mask), row(region_id), block_fill, row(cell_area))
    return region, mean, count.reshape(REGIONS)


def solution(mesh):
    body = functools.partial(shards, mesh.shape["cells"], mesh.shape["members"])
    return jax.shard_map(
        body,
        mesh=mesh,
        in_specs=(
            P("members", None, "cells"),
            P("cells"),
            P("cells"),
            P("cells"),
            P("cells"),
            P("cells"),
        ),
        out_specs=(P("members", None, None), P("members", "cells"), P()),
        check_vma=False,
    )
```
